32 devices in a mesh: seq: 8 (over y, x, core), head: 4 (over z).
Axes of the slice: x: 2, y: 2, z: 4, core: 2. Of those that a mesh axis runs over, the one named last changes fastest.
Arguments:
- latent: bfloat16 [1024, 1024], P('seq'), may hold values from -15 to 15
- probe: bfloat16 [1024, 1024], P('seq'), may hold values from -6 to 6
- time_embed: float32 [1024], replicated, may hold values from -6 to 6
- gain_attn: float32 [1024], replicated, may hold values from 0.1 to 1.9
- w_query: bfloat16 [1024, 1024], P(None, 'head'), may hold values from -0.625 to 0.625
- w_key: bfloat16 [1024, 1024], P(None, 'head'), may hold values from -11 to 11
- w_value: bfloat16 [1024, 1024], P(None, 'head'), may hold values from -0.1875 to 0.1875
- w_out: bfloat16 [1024, 1024], P('head'), may hold values from -0.1875 to 0.1875
- gain_mlp: float32 [1024], replicated, may hold values from 0.1 to 1.9
- w_in: bfloat16 [1024, 4096], P(None, 'head'), may hold values from -0.1875 to 0.1875
- w_down: bfloat16 [4096, 1024], P('head'), may hold values from -0.09375 to 0.09375
Outputs:
- latent_end: float32 [1024, 1024], P('seq')
- frame_trace: float32 [1024], P('seq')
- frame_logp: float32 [1024], P('seq')
- mean_logp: float32 [], replicated
The draws below stay inside these ranges and needn't reach their ends.
All inputs are finite; a program needn't handle non-finite values.
Results may differ from the reference program's by a relative error of at most 0.03.
The reference program's roundings to bfloat16 on the way count: a program that leaves them out, or rounds other values in their place, can miss the bound.
Values may be sent and summed in bfloat16 or wider, within the bound.
No kernel may reach another device: no remote copies, remote signals or barrier semaphores. Data moves between devices by JAX's collectives and lax.ppermute only.
A program may use at most 64 MiB of HBM per device.

```python
import math
import jax
import jax.numpy as jnp
from jax import lax

D = 1024
HEADS = 16
HEAD_DIM = 64
FF = 4096
STEPS = 2
FRAMES = 1024


def weight_pair(key):
    base = jax.random.fold_in(key, 11)
    first, second = jax.random.split(base, 2)
    query_weight = jnp.clip(jax.random.normal(first, (D, D), jnp.float32), -5.0, 5.0) * D ** (-0.5)
    noise = jnp.clip(jax.random.normal(second, (D, D), jnp.float32), -5.0, 5.0) * D ** (-0.5)
    key_weight = 3.0 * noise
    return (query_weight, key_weight)


def draw_w_query(key, part):
    return weight_pair(key)[0].astype(jnp.bfloat16)


def draw_w_key(key, part):
    return weight_pair(key)[1].astype(jnp.bfloat16)


def draw_latent(key, part):
    base = jax.random.fold_in(key, 23)
    position = jnp.arange(FRAMES, dtype=jnp.float32) / max(FRAMES - 1, 1)
    entries = jnp.clip(jax.random.normal(base, (FRAMES, D), jnp.float32), -5.0, 5.0)
    ramp = 1.0 + 2.0 * position
    return (entries * ramp[:, None]).astype(jnp.bfloat16)


def steps_of(key, extent, shards, low, high):
    factor_of, own = 1.0, jax.random.fold_in(key, 6)
    for dim, blocks in shards:
        heights = jnp.exp(jax.random.uniform(jax.random.fold_in(own, dim), (blocks,), jnp.float32, low / len(shards), high / len(shards)))
        factor_of = factor_of * jnp.repeat(heights, extent[dim] // blocks).reshape([-1 if axis == dim else 1 for axis in range(len(extent))])
    return factor_of


def normal_values(stream_key, extent, deviation, most, shards=(), held_as=jnp.bfloat16):
    array = jax.random.normal(stream_key, extent, jnp.float32) * deviation
    if len(shards) > 0:
        array = steps_of(stream_key, extent, shards, -0.22, 0.18) * array
    return jnp.clip(array, min=-most, max=most).astype(held_as)


def setup_inputs(seed: int = 0) -> dict:
    key_of = jax.random.split(jax.random.key(seed), 12)
    latent = draw_latent(jax.random.fold_in(key_of[11], 71), 0)
    probe = normal_values(key_of[1], (FRAMES, D), 1.0, 6.0, ((0, 8),))
    time_embed = normal_values(key_of[2], (D,), 1.0, 6.0, (), jnp.float32)
    gain_attn = jnp.clip(1.0 + 0.18 * jax.random.normal(key_of[3], (D,), jnp.float32), 0.1, 1.9)
    w_query = draw_w_query(jax.random.fold_in(key_of[11], 71), 0)
    w_key = draw_w_key(jax.random.fold_in(key_of[11], 71), 0)
    w_value = normal_values(key_of[6], (D, D), D ** -0.5, 0.1875, ((1, 4),))
    w_out = normal_values(key_of[7], (D, D), D ** -0.5, 0.1875, ((0, 4),))
    gain_mlp = jnp.clip(1.0 + 0.18 * jax.random.normal(key_of[8], (D,), jnp.float32), 0.1, 1.9)
    w_in = normal_values(key_of[9], (D, FF), D ** -0.5, 0.1875, ((1, 4),))
    w_down = normal_values(key_of[10], (FF, D), FF ** -0.5, 0.09375, ((0, 4),))
    return dict(latent=latent, probe=probe, time_embed=time_embed, gain_attn=gain_attn, w_query=w_query, w_key=w_key, w_value=w_value, w_out=w_out, gain_mlp=gain_mlp, w_in=w_in, w_down=w_down)


EPSILON = 1e-05
GELU_COEF = 0.044715
ROOT_TWO_PI = math.sqrt(2.0 / math.pi)

def norm_pair(values, tangent, norm_gain):
    meansq = lax.optimization_barrier(jnp.mean(values * values, axis=-1, keepdims=True)) + EPSILON
    inverse = lax.rsqrt(meansq)
    inner_mean = lax.optimization_barrier(jnp.mean(values * tangent, axis=-1, keepdims=True))
    primal = values * inverse * norm_gain
    derived = (tangent * inverse - values * inverse ** 3 * inner_mean) * norm_gain
    return (primal.astype(jnp.bfloat16), derived.astype(jnp.bfloat16))

def gelu_pair(pre_act, tangent):
    cubic_arg = pre_act + GELU_COEF * pre_act ** 3
    tanh_value = jnp.tanh(ROOT_TWO_PI * cubic_arg)
    output = 0.5 * pre_act * (1.0 + tanh_value)
    slope_value = 0.5 * (1.0 + tanh_value) + 0.5 * pre_act * (1.0 - tanh_value * tanh_value) * ROOT_TWO_PI * (1.0 + 3.0 * GELU_COEF * pre_act * pre_act)
    return (output.astype(jnp.bfloat16), (slope_value * tangent).astype(jnp.bfloat16))

def attention(queries, query_tang, keys, vals, key_tang, val_tang):
    scale = HEAD_DIM ** (-0.5)

    def heads_of(matrix):
        return matrix.astype(jnp.float32).reshape(FRAMES, HEADS, HEAD_DIM)
    keys_all = heads_of(keys)
    vals_all = heads_of(vals)
    key_tang_all = heads_of(key_tang)
    val_tang_all = heads_of(val_tang)
    block = math.gcd(FRAMES, 512)

    def one_block(pair):
        block_queries, block_tang = pair
        scores = jnp.einsum('bhd,shd->hbs', block_queries, keys_all) * scale
        score_tang = (jnp.einsum('bhd,shd->hbs', block_tang, keys_all) + jnp.einsum('bhd,shd->hbs', block_queries, key_tang_all)) * scale
        row_top = lax.optimization_barrier(jnp.max(scores, axis=-1, keepdims=True))
        weights = jnp.exp(scores - row_top)
        total = lax.optimization_barrier(jnp.sum(weights, axis=-1))
        weighted = weights * score_tang
        carried = lax.optimization_barrier(jnp.sum(weighted, axis=-1))
        rounded = lax.optimization_barrier(weights.astype(jnp.bfloat16)).astype(jnp.float32)
        rounded_tang = lax.optimization_barrier(weighted.astype(jnp.bfloat16)).astype(jnp.float32)
        acc_primal = jnp.einsum('hbs,shd->bhd', rounded, vals_all)
        acc_tang = jnp.einsum('hbs,shd->bhd', rounded_tang, vals_all) + jnp.einsum('hbs,shd->bhd', rounded, val_tang_all)
        total_t = jnp.transpose(total)[:, :, None]
        carried_t = jnp.transpose(carried)[:, :, None]
        primal = acc_primal / total_t
        tangent = acc_tang / total_t - carried_t / total_t * primal
        return (primal.astype(jnp.bfloat16), tangent.astype(jnp.bfloat16))
    query_blocks = heads_of(queries).reshape(FRAMES // block, block, HEADS, HEAD_DIM)
    tang_blocks = heads_of(query_tang).reshape(FRAMES // block, block, HEADS, HEAD_DIM)
    head_out, head_tang = lax.map(one_block, (query_blocks, tang_blocks))
    return (head_out.reshape(FRAMES, D), head_tang.reshape(FRAMES, D))

def vector_field(inputs, direction, gain_attn, w_query, w_key, w_value, w_out, gain_mlp, w_in, w_down):
    normed, normed_tang = norm_pair(inputs, direction, gain_attn)

    def project(weight):
        primal = jnp.dot(normed, weight, preferred_element_type=jnp.float32).astype(jnp.bfloat16)
        tangent = jnp.dot(normed_tang, weight, preferred_element_type=jnp.float32).astype(jnp.bfloat16)
        return (primal, tangent)
    queries, query_tang = project(w_query)
    keys, key_tang = project(w_key)
    vals, val_tang = project(w_value)
    head_out, head_tang = attention(queries, query_tang, keys, vals, key_tang, val_tang)
    attn = jnp.dot(head_out, w_out, preferred_element_type=jnp.float32)
    attn_tang = jnp.dot(head_tang, w_out, preferred_element_type=jnp.float32)
    middle = inputs + attn
    middle_tang = direction + attn_tang
    normed_mlp, normed_mlp_tang = norm_pair(middle, middle_tang, gain_mlp)
    pre_act = jnp.dot(normed_mlp, w_in, preferred_element_type=jnp.float32)
    pre_tang = jnp.dot(normed_mlp_tang, w_in, preferred_element_type=jnp.float32)
    activ, activ_tang = gelu_pair(pre_act, pre_tang)
    mlp_out = jnp.dot(activ, w_down, preferred_element_type=jnp.float32)
    mlp_tang = jnp.dot(activ_tang, w_down, preferred_element_type=jnp.float32)
    return (attn + mlp_out, attn_tang + mlp_tang)

def reference(latent, probe, time_embed, gain_attn, w_query, w_key, w_value, w_out, gain_mlp, w_in, w_down):
    state = latent.astype(jnp.float32)
    direction = probe.astype(jnp.float32)
    trace = jnp.zeros((FRAMES,), jnp.float32)
    for euler_step in range(STEPS):
        inputs = state + euler_step / STEPS * time_embed
        field, field_tang = vector_field(inputs, direction, gain_attn, w_query, w_key, w_value, w_out, gain_mlp, w_in, w_down)
        trace = trace + lax.optimization_barrier(jnp.sum(direction * field_tang, axis=-1)) / (STEPS * D)
        state = state + field / STEPS
    frame_logp = trace - 0.5 * lax.optimization_barrier(jnp.sum(state * state, axis=-1)) / D - 0.5 * math.log(2.0 * math.pi)
    mean_logp = jnp.mean(frame_logp)
    return (state, trace, frame_logp, mean_logp)
```

```python
import functools
import math

import jax
import jax.numpy as jnp
from jax import lax
from jax.experimental import pallas as pl
from jax.experimental.pallas import tpu as pltpu
from jax.sharding import PartitionSpec as P

HEAD_DIM = 64
STEPS = 2
EPSILON = 1e-05
GELU_COEF = 0.044715
ROOT_TWO_PI = math.sqrt(2.0 / math.pi)


VMEM = pl.BlockSpec(memory_space=pltpu.VMEM)
SMEM = pl.BlockSpec(memory_space=pltpu.SMEM)
PARAMS = pltpu.CompilerParams(vmem_limit_bytes=56 * 1024 * 1024)


def call(kernel, outs, scalars, *operands, scratch=()):
    return pl.pallas_call(
        kernel,
        out_shape=outs,
        in_specs=[SMEM] * len(scalars) + [VMEM] * len(operands),
        out_specs=jax.tree.map(lambda _: VMEM, outs),
        scratch_shapes=scratch,
        compiler_params=PARAMS,
    )(*scalars, *operands)


def norm_pair(values, tangent, norm_gain):
    meansq = jnp.mean(values * values, axis=-1, keepdims=True) + EPSILON
    inverse = lax.rsqrt(meansq)
    inner_mean = jnp.mean(values * tangent, axis=-1, keepdims=True)
    primal = values * inverse * norm_gain
    derived = (tangent * inverse - values * inverse**3 * inner_mean) * norm_gain
    return (primal.astype(jnp.bfloat16), derived.astype(jnp.bfloat16))


def gelu_pair(pre_act, tangent):
    cubic_arg = pre_act + GELU_COEF * pre_act**3
    tanh_value = jnp.tanh(ROOT_TWO_PI * cubic_arg)
    output = 0.5 * pre_act * (1.0 + tanh_value)
    slope_value = 0.5 * (1.0 + tanh_value) + 0.5 * pre_act * (
        1.0 - tanh_value * tanh_value
    ) * ROOT_TWO_PI * (1.0 + 3.0 * GELU_COEF * pre_act * pre_act)
    return (output.astype(jnp.bfloat16), (slope_value * tangent).astype(jnp.bfloat16))


def dot(a, b):
    return jnp.dot(a, b, preferred_element_type=jnp.float32)


def norm_project(values, probe_ref, gain_ref, wk_ref, wv_ref, pair_ref, kv_ref):
    rows = values.shape[0]
    primal, derived = norm_pair(values, probe_ref[...].astype(jnp.float32), gain_ref[...])
    pair_ref[:rows, :] = primal
    pair_ref[rows:, :] = derived
    pair = pair_ref[...]
    keys = dot(pair, wk_ref[...]).astype(jnp.bfloat16)
    vals = dot(pair, wv_ref[...]).astype(jnp.bfloat16)
    for h in range(keys.shape[1] // HEAD_DIM):
        col = slice(h * HEAD_DIM, (h + 1) * HEAD_DIM)
        base = h * 4 * HEAD_DIM
        kv_ref[:, base : base + 4 * HEAD_DIM] = jnp.concatenate(
            [keys[:rows, col], keys[rows:, col], vals[:rows, col], vals[rows:, col]], axis=1
        )


def first_kernel(latent_ref, probe_ref, gain_ref, wk_ref, wv_ref, pair_ref, kv_ref):
    values = latent_ref[...].astype(jnp.float32)
    norm_project(values, probe_ref, gain_ref, wk_ref, wv_ref, pair_ref, kv_ref)


def update_state(me, state_ref, attn_ref, piece_refs, out_ref):
    part = piece_refs[0].shape[0]
    for k, piece in enumerate(piece_refs):
        at = pl.ds(pl.multiple_of((me ^ k) * part, part), part)
        field = attn_ref[at, :] + piece[...].astype(jnp.float32)
        out_ref[at, :] = state_ref[at, :].astype(jnp.float32) + field / STEPS


def next_kernel(fraction, n, me_ref, state_ref, attn_ref, *refs):
    pieces = refs[:n]
    embed_ref, probe_ref, gain_ref, wk_ref, wv_ref, state_out, inputs_out, pair_ref, kv_ref = refs[n:]
    update_state(me_ref[0], state_ref, attn_ref, pieces, state_out)
    values = state_out[...] + fraction * embed_ref[...]
    inputs_out[...] = values
    norm_project(values, probe_ref, gain_ref, wk_ref, wv_ref, pair_ref, kv_ref)


def as_row(column):
    return jnp.transpose(jnp.broadcast_to(column, (column.shape[0], 128)))[:8]


def last_kernel(n, me_ref, state_ref, attn_ref, *refs):
    pieces = refs[:n]
    trace_refs = refs[n : 2 * n]
    state_out, trace_out, logp_out = refs[2 * n :]
    update_state(me_ref[0], state_ref, attn_ref, pieces, state_out)
    state = state_out[...]
    width = state.shape[1]
    trace = tree_sum([t[...] for t in trace_refs]) / (STEPS * width)
    square = as_row(jnp.sum(state * state, axis=-1, keepdims=True))
    trace_out[...] = trace
    logp_out[...] = trace - 0.5 * square / width - 0.5 * math.log(2.0 * math.pi)


def query_kernel(pair_ref, wq_ref, a_ref):
    rows = pair_ref.shape[0] // 2
    queries = dot(pair_ref[...], wq_ref[...]).astype(jnp.bfloat16)
    zeros = jnp.zeros((rows, HEAD_DIM), jnp.bfloat16)
    for h in range(queries.shape[1] // HEAD_DIM):
        col = slice(h * HEAD_DIM, (h + 1) * HEAD_DIM)
        base = h * 2 * HEAD_DIM
        both = slice(base, base + 2 * HEAD_DIM)
        a_ref[:rows, both] = jnp.concatenate([queries[:rows, col], zeros], axis=1)
        a_ref[rows:, both] = jnp.concatenate([queries[rows:, col], queries[:rows, col]], axis=1)


def attention_kernel(a_ref, *refs):
    pieces, out_ref = refs[:-1], refs[-1]
    rows = a_ref.shape[0] // 2
    scale = HEAD_DIM ** (-0.5)
    contract = (((1,), (1,)), ((), ()))
    for h in range(a_ref.shape[1] // (2 * HEAD_DIM)):
        queries = a_ref[:, h * 2 * HEAD_DIM : (h + 1) * 2 * HEAD_DIM]
        base = h * 4 * HEAD_DIM
        keys = jnp.concatenate([p[:, base : base + 2 * HEAD_DIM] for p in pieces], axis=0)
        vals = jnp.concatenate(
            [p[:, base + 2 * HEAD_DIM : base + 4 * HEAD_DIM] for p in pieces], axis=0
        )
        both = lax.dot_general(queries, keys, contract, preferred_element_type=jnp.float32) * scale
        scores, score_tang = both[:rows], both[rows:]
        weights = jnp.exp(scores - jnp.max(scores, axis=-1, keepdims=True))
        total = jnp.sum(weights, axis=-1, keepdims=True)
        weighted = weights * score_tang
        carried = jnp.sum(weighted, axis=-1, keepdims=True)
        stacked = jnp.concatenate(
            [weights.astype(jnp.bfloat16), weighted.astype(jnp.bfloat16)], axis=0
        )
        acc = dot(stacked, vals)
        primal = acc[:rows, :HEAD_DIM] / total
        tangent = (acc[rows:, :HEAD_DIM] + acc[:rows, HEAD_DIM:]) / total - carried / total * primal
        out_ref[:rows, h * HEAD_DIM : (h + 1) * HEAD_DIM] = primal.astype(jnp.bfloat16)
        out_ref[rows:, h * HEAD_DIM : (h + 1) * HEAD_DIM] = tangent.astype(jnp.bfloat16)


def tree_sum(terms):
    while len(terms) > 1:
        terms = [a + b for a, b in zip(terms[0::2], terms[1::2])]
    return terms[0]


def mlp_kernel(n, me_ref, inputs_ref, probe_ref, gain_ref, *refs):
    heads = refs[:n]
    outs_w = refs[n : 2 * n]
    w_in_ref, w_down_ref = refs[2 * n : 2 * n + 2]
    attn_ref, trace_ref, own_ref = refs[2 * n + 2 : 2 * n + 5]
    send_refs = refs[2 * n + 5 : 3 * n + 4]
    partial_ref = refs[-1]
    rows = inputs_ref.shape[0]
    me = me_ref[0]
    probe = probe_ref[...].astype(jnp.float32)
    attn = tree_sum([dot(h[...], w[...]) for h, w in zip(heads, outs_w)])
    attn_ref[...] = attn[:rows]
    attn_tang = attn[rows:]
    middle = inputs_ref[...].astype(jnp.float32) + attn[:rows]
    normed, normed_tang = norm_pair(middle, probe + attn_tang, gain_ref[...])
    w_in = w_in_ref[...]
    act, act_tang = gelu_pair(dot(normed, w_in), dot(normed_tang, w_in))
    partial_ref[...] = dot(act, w_down_ref[...])
    part = rows // n
    for k in range(n):
        at = pl.ds(pl.multiple_of((me ^ k) * part, part), part)
        if k == 0:
            own_ref[...] = partial_ref[at, :]
        else:
            send_refs[k - 1][...] = partial_ref[at, :].astype(jnp.bfloat16)
    mlp_tang = dot(act_tang, w_down_ref[...])
    column = jnp.sum(probe * (attn_tang * (1.0 / n) + mlp_tang), axis=-1, keepdims=True)
    trace_ref[...] = as_row(column)


def swap(value, axis, k):
    size = lax.axis_size(axis)
    return lax.ppermute(value, axis, [(i, i ^ k) for i in range(size)])


def everyone(value, axis):
    return [value] + [swap(value, axis, k) for k in range(1, lax.axis_size(axis))]


def gather_kv(kv):
    size = lax.axis_size("seq")
    pieces = [kv] + [swap(kv, "seq", k) for k in range(2, size, 2)]
    return pieces + [swap(p, "seq", 1) for p in pieces]


def gather_out(w_out):
    n = lax.axis_size("head")
    half = w_out.shape[0] // 2
    side = lax.axis_index("seq") % 2
    mine = lax.dynamic_slice_in_dim(w_out, side * half, half, 0)
    result = [w_out]
    for k in range(1, n):
        near = swap(mine, "head", k)
        far = swap(near, "seq", 1)
        low = jnp.where(side == 0, near, far)
        high = jnp.where(side == 0, far, near)
        result.append(jnp.concatenate([low, high], axis=0))
    return result


def per_device(
    latent, probe, time_embed, gain_attn, w_query, w_key, w_value, w_out, gain_mlp, w_in, w_down
):
    rows, width = latent.shape
    local = w_query.shape[1]
    n = lax.axis_size("head")
    part = rows // n
    f32, bf16 = jnp.float32, jnp.bfloat16
    shape = jax.ShapeDtypeStruct
    me = lax.axis_index("head").astype(jnp.int32).reshape(1)
    gain_attn, gain_mlp, embed = (v.reshape(1, width) for v in (gain_attn, gain_mlp, time_embed))
    pair_shape = shape((2 * rows, width), bf16)
    kv_shape = shape((rows, 4 * local), bf16)
    state = latent
    inputs = latent
    traces = []
    pair, kv = call(
        first_kernel, (pair_shape, kv_shape), (), latent, probe, gain_attn, w_key, w_value
    )
    out_pieces = gather_out(w_out)
    for step in range(STEPS):
        if step > 0:
            state, inputs, pair, kv = call(
                functools.partial(next_kernel, step / STEPS, n),
                (shape((rows, width), f32), shape((rows, width), f32), pair_shape, kv_shape),
                (me,),
                state, attn, *mlp_pieces, embed, probe, gain_attn, w_key, w_value,
            )
        kv_pieces = gather_kv(kv)
        queries = call(query_kernel, shape((2 * rows, 2 * local), bf16), (), pair, w_query)
        head_out = call(
            attention_kernel, shape((2 * rows, local), bf16), (), queries, *kv_pieces
        )
        head_pieces = everyone(head_out, "head")
        attn, trace_part, own, *sends = call(
            functools.partial(mlp_kernel, n),
            (shape((rows, width), f32), shape((8, rows), f32), shape((part, width), f32))
            + (shape((part, width), bf16),) * (n - 1),
            (me,),
            inputs, probe, gain_mlp, *head_pieces, *out_pieces, w_in, w_down,
            scratch=[pltpu.VMEM((rows, width), f32)],
        )
        traces.append(trace_part)
        landed = [swap(send, "head", k + 1).astype(f32) for k, send in enumerate(sends)]
        mlp_pieces = everyone(tree_sum([own] + landed).astype(bf16), "head")
    trace_pieces = everyone(sum(traces), "head")
    state, trace, logp = call(
        functools.partial(last_kernel, n),
        (shape((rows, width), f32), shape((8, rows), f32), shape((8, rows), f32)),
        (me,),
        state, attn, *mlp_pieces, *trace_pieces,
    )
    trace, logp = trace[0], logp[0]
    sums = everyone(jnp.broadcast_to(jnp.sum(logp), (8, 128)), "seq")
    mean_logp = tree_sum(sums)[0, 0] / (rows * lax.axis_size("seq"))
    return (state, trace, logp, mean_logp)


def solution(mesh):
    return jax.shard_map(
        per_device,
        mesh=mesh,
        in_specs=(
            P("seq", None),
            P("seq", None),
            P(),
            P(),
            P(None, "head"),
            P(None, "head"),
            P(None, "head"),
            P("head", None),
            P(),
            P(None, "head"),
            P("head", None),
        ),
        out_specs=(P("seq", None), P("seq"), P("seq"), P()),
        check_vma=False,
    )
```
